256 devices in a mesh: group: 32 (over x, z), tensor: 8 (over y, core).
Axes of the slice: x: 4, y: 4, z: 8, core: 2. Of those that a mesh axis runs over, the one named last changes fastest.
Arguments:
- queries: bfloat16 [1024, 64, 5120], P('group', None, 'tensor'), may hold values from -15 to 15
- prefix_keys: bfloat16 [64, 1024, 1024], P('group', None, 'tensor'), may hold values from -200 to 200
- prefix_values: bfloat16 [64, 1024, 1024], P('group', None, 'tensor'), may hold values from -6 to 6
- slot_of_prompt: int32 [64], replicated, may hold values from 0 to 63, as said below
- prompt_of: int32 [1024], P('group'), may hold values from 0 to 63, as said below
- lengths: int32 [1024], P('group'), may hold values from 1 to 64
Outputs:
- attended: bfloat16 [1024, 64, 5120], P('group', 'tensor')
The draws below stay inside these ranges and needn't reach their ends.
Inputs may be any that keep to these rules, and one draw needn't show every extreme that they name: A permutation: prompt p's keys and values lie in row slot_of_prompt[p] of the prefix arrays, and that row belongs to group index slot_of_prompt[p] // 2. `prompt_of`: of the 32 completions on one group index, at most 2 have prompts cached on any one group index, and on every group index some group index caches the prompts of exactly 2 of them.
All inputs are finite; a program needn't handle non-finite values.
Results may differ from the reference program's by a relative error of at most 0.012.
Values may be sent and summed in bfloat16 or wider, within the bound.
No kernel may reach another device: no remote copies, remote signals or barrier semaphores. Data moves between devices by JAX's collectives and lax.ppermute only.
A program may use at most 64 MiB of HBM per device.

```python
import math
import jax
import jax.numpy as jnp
from jax import lax

D = 5120
HEADS = 40
KV_HEADS = 8
HEAD = 128
PREFIX = 1024
COMP = 64
CAPC = 2
PPG = 2
CPD = 32
COMPLETIONS = 1024
PROMPTS = 64


def routing_tables(key):
    base = jax.random.fold_in(key, 4217)
    first_key, second_key = jax.random.split(base, 2)
    slot_of_prompt = jax.random.permutation(first_key, PROMPTS).astype(jnp.int32)
    prompt_at = jnp.argsort(slot_of_prompt, stable=True).astype(jnp.int32)
    blocks = COMPLETIONS // CPD
    block_keys = jax.random.split(second_key, blocks)

    def one_block(block_key):
        key_spare, key_order, key_offset, key_local = jax.random.split(block_key, 4)
        spare = CAPC + jax.random.permutation(key_spare, blocks * CAPC - CAPC)
        chosen = jnp.concatenate([jnp.arange(CAPC), spare[:CPD - CAPC]])
        chosen = jax.random.permutation(key_order, chosen)
        offset = jax.random.randint(key_offset, (), 0, blocks)
        owner_group = (chosen // CAPC + offset) % blocks
        local_rows = jax.random.randint(key_local, (CPD,), 0, PPG)
        return owner_group * PPG + local_rows
    cache_slots = jax.vmap(one_block)(block_keys).reshape(COMPLETIONS)
    prompt_of = prompt_at[cache_slots].astype(jnp.int32)
    return (slot_of_prompt, prompt_of)


def draw_slot_of_prompt(key, part):
    return routing_tables(key)[0]


def draw_prompt_of(key, part):
    return routing_tables(key)[1]


def draw_prefix_keys(key, part):
    base = jax.random.fold_in(key, 913)
    key_base = jax.random.fold_in(base, 0)
    entries = jax.random.normal(key_base, (PROMPTS, PREFIX, KV_HEADS, HEAD), jnp.float32)
    entries = jnp.clip(entries, -200.0, 200.0)
    return entries.reshape(PROMPTS, PREFIX, KV_HEADS * HEAD).astype(jnp.bfloat16)


def place_ends(array, stream_key, smallest, largest):
    dims = array.shape
    spot = [jax.random.randint(jax.random.fold_in(stream_key, axis), (), 0, dims[axis]) for axis in range(len(dims))]
    array = array.at[tuple(spot)].set(smallest)
    longest = dims.index(max(dims))
    spot[longest] = (spot[longest] + 1) % dims[longest]
    return array.at[tuple(spot)].set(largest)


def shard_levels(stream_key, shape, cuts, smallest, largest):
    level = 1.0
    for position, blocks in cuts:
        draws = jax.random.uniform(jax.random.fold_in(jax.random.fold_in(stream_key, 6), position), (blocks,), jnp.float32, smallest / len(cuts), largest / len(cuts))
        level = level * jnp.repeat(jnp.exp(draws), shape[position] // blocks).reshape((-1,) + (1,) * (len(shape) - 1 - position))
    return level


def bell_draw(rng, shape, deviation, limit, pieces=(), kind=jnp.bfloat16):
    values = deviation * jax.random.normal(rng, shape, jnp.float32)
    if pieces:
        values = values * shard_levels(rng, shape, pieces, -0.22, 0.18)
    return jnp.clip(values, -limit, limit).astype(kind)


def setup_inputs(seed: int = 0) -> dict:
    key_list = jax.random.split(jax.random.key(seed), 7)
    queries = bell_draw(key_list[0], (COMPLETIONS, COMP, D), 2.5, 15.0, ((0, 32), (2, 8)))
    prefix_keys = draw_prefix_keys(jax.random.fold_in(key_list[6], 71), 0)
    prefix_values = bell_draw(key_list[2], (PROMPTS, PREFIX, KV_HEADS * HEAD), 1.0, 6.0, ((0, 32), (2, 8)))
    slot_of_prompt = draw_slot_of_prompt(jax.random.fold_in(key_list[6], 71), 0)
    prompt_of = draw_prompt_of(jax.random.fold_in(key_list[6], 71), 0)
    lengths = place_ends(jax.random.randint(key_list[5], (COMPLETIONS,), 1, COMP + 1), jax.random.fold_in(key_list[5], 1), 1, COMP).astype(jnp.int32)
    return dict(queries=queries, prefix_keys=prefix_keys, prefix_values=prefix_values, slot_of_prompt=slot_of_prompt, prompt_of=prompt_of, lengths=lengths)


rotary_base = 1000000.0

def rotary(head_rows, positions):
    half_dim = head_rows.shape[-1] // 2
    frequencies = rotary_base ** (-(jnp.arange(half_dim, dtype=jnp.float32) * 2.0 / head_rows.shape[-1]))
    angles = positions[:, None] * frequencies[None, :]
    cos_table = jnp.cos(angles)[:, None, :]
    sin_table = jnp.sin(angles)[:, None, :]
    first_half = head_rows[..., :half_dim]
    second_half = head_rows[..., half_dim:]
    return jnp.concatenate([first_half * cos_table - second_half * sin_table, second_half * cos_table + first_half * sin_table], axis=-1)

def reference(queries, prefix_keys, prefix_values, slot_of_prompt, prompt_of, lengths):
    positions = (PREFIX + jnp.arange(COMP)).astype(jnp.float32)
    cache_rows = slot_of_prompt[prompt_of].astype(jnp.int32)
    per_kv = HEADS // KV_HEADS
    scaling = 1.0 / math.sqrt(HEAD)
    highest = lax.Precision.HIGHEST

    def single(inputs):
        query_rows, cache_row, length = inputs
        roped = rotary(query_rows.astype(jnp.float32).reshape(COMP, HEADS, HEAD), positions).astype(jnp.bfloat16)
        grouped = roped.astype(jnp.float32).reshape(COMP, KV_HEADS, per_kv, HEAD)
        cached_keys = lax.dynamic_index_in_dim(prefix_keys, cache_row, 0, keepdims=False).astype(jnp.float32).reshape(PREFIX, KV_HEADS, HEAD)
        cached_values = lax.dynamic_index_in_dim(prefix_values, cache_row, 0, keepdims=False).astype(jnp.float32).reshape(PREFIX, KV_HEADS, HEAD)
        scores = jnp.einsum('rkgd,pkd->kgrp', grouped, cached_keys, precision=highest) * scaling
        peak = lax.optimization_barrier(jnp.max(scores, axis=-1, keepdims=True))
        weights = jnp.exp(scores - peak)
        denominator = lax.optimization_barrier(jnp.sum(weights, axis=-1))
        probabilities = weights.astype(jnp.bfloat16).astype(jnp.float32)
        weighted = jnp.einsum('kgrp,pkd->rkgd', probabilities, cached_values, precision=highest)
        attended = (weighted / jnp.transpose(denominator, (2, 0, 1))[..., None]).astype(jnp.bfloat16).reshape(COMP, D)
        live_rows = jnp.arange(COMP) < length
        return jnp.where(live_rows[:, None], attended, jnp.zeros_like(attended))
    return lax.map(single, (queries, cache_rows, lengths))
```

```python
import functools
import math

import jax
import jax.numpy as jnp
import numpy as np
from jax import lax
from jax.experimental import pallas as pl
from jax.experimental.pallas import tpu as pltpu
from jax.sharding import Mesh, PartitionSpec as P


HEAD = 128
CAPC = 2
ROTARY_BASE = 1000000.0
VMEM = 67043328
GROUPS_Z = 8
NEAR = 5
TURN = 4
TAIL = 16


def rotary_tables(first_position, rows):
    half = HEAD // 2
    frequencies = np.float32(ROTARY_BASE) ** (
        -(np.arange(half, dtype=np.float32) * np.float32(2.0) / np.float32(HEAD))
    )
    positions = np.arange(first_position, first_position + rows).astype(np.float32)
    angles = (positions[:, None] * frequencies[None, :]).astype(np.float32).astype(np.float64)
    cos, sin = np.cos(angles), np.sin(angles)
    return np.stack(
        [np.concatenate([cos, cos], axis=1), np.concatenate([-sin, sin], axis=1)]
    ).astype(np.float32)


def route(prompt, slot_ref, counts_ref, my_z):
    cache_slot = slot_ref[prompt]
    owner = cache_slot // 2
    row = cache_slot - owner * 2
    owner_x = owner // GROUPS_Z
    distance = lax.rem(owner - owner_x * GROUPS_Z - my_z + GROUPS_Z, GROUPS_Z)
    place = jnp.where(
        distance == 0, 0, jnp.where(distance <= 4, 2 * distance - 1, 2 * (GROUPS_Z - distance))
    )
    arrival = counts_ref[owner]
    counts_ref[owner] = arrival + 1
    return owner_x, place * CAPC + arrival, row


def pack_kernel(
    low, high, z_ref, slots_ref, prompts_ref, lengths_ref, queries_ref, tables_ref, sent_ref,
    held, staged, tables, tagged, slot_ref, prompt_ref, length_ref, counts_ref,
    to_x_ref, to_slot_ref, in_sems, out_sems, small_sems, tag_sem,
):
    items, rows, width = queries_ref.shape
    heads = width // HEAD
    tagging = sent_ref.shape[1] > (high - low) * rows
    smalls = [
        pltpu.make_async_copy(source, target, small_sems.at[index])
        for index, (source, target) in enumerate(
            (
                (slots_ref, slot_ref), (prompts_ref, prompt_ref), (lengths_ref, length_ref),
                (tables_ref, tables),
            )
        )
    ]
    for copy in smalls:
        copy.start()
    my_z = z_ref[0]
    for group in range(counts_ref.shape[0]):
        counts_ref[group] = 0
    line = lax.broadcasted_iota(jnp.int32, (8, HEAD), 0)
    lane = lax.broadcasted_iota(jnp.int32, (8, HEAD), 1)
    for copy in smalls:
        copy.wait()

    def plan(item, carry):
        found, tags = carry
        owner_x, slot, row = route(prompt_ref[item], slot_ref, counts_ref, my_z)
        inside = (slot >= low) & (slot < high)

        @pl.when(inside)
        def _():
            pltpu.make_async_copy(queries_ref.at[item], held.at[found], in_sems.at[found]).start()
            to_x_ref[found] = owner_x
            to_slot_ref[found] = slot - low

        if tagging:
            tags = jnp.where((line == owner_x) & (lane == slot), row + 1, tags)
            tags = jnp.where((line == owner_x) & (lane == slot + 64), length_ref[item], tags)
        return found + jnp.where(inside, 1, 0), tags

    found, tags = lax.fori_loop(0, items, plan, (0, jnp.zeros((8, HEAD), jnp.int32)))
    tail_copies = []
    if tagging:
        tags = tags.astype(jnp.float32)
        for owner_x in range(sent_ref.shape[0]):
            tagged[owner_x] = jnp.broadcast_to(tags[owner_x : owner_x + 1], (TAIL, HEAD)).astype(
                jnp.bfloat16
            )
            tail_copies.append(
                pltpu.make_async_copy(
                    tagged.at[owner_x],
                    sent_ref.at[owner_x, pl.ds((high - low) * rows, TAIL), pl.ds(0, HEAD)],
                    tag_sem.at[owner_x],
                )
            )
            tail_copies[-1].start()

    def turn(step, carry):
        for inner in range(TURN):
            index = step * TURN + inner

            @pl.when(index < found)
            def _(index=index):
                pltpu.make_async_copy(queries_ref.at[0], held.at[index], in_sems.at[index]).wait()

        for inner in range(TURN):
            index = step * TURN + inner
            for head in range(heads):
                part = held[index, :, head * HEAD : (head + 1) * HEAD].astype(jnp.float32)
                turned = part * tables[0] + pltpu.roll(part, HEAD // 2, 1) * tables[1]
                staged[index, :, head * HEAD : (head + 1) * HEAD] = turned.astype(jnp.bfloat16)
        for inner in range(TURN):
            index = step * TURN + inner

            @pl.when(index < found)
            def _(index=index):
                at = pl.ds(pl.multiple_of(to_slot_ref[index] * rows, rows), rows)
                pltpu.make_async_copy(
                    staged.at[index], sent_ref.at[to_x_ref[index], at], out_sems.at[index]
                ).start()

        return carry

    lax.fori_loop(0, (found + TURN - 1) // TURN, turn, 0)

    def leave(index, carry):
        pltpu.make_async_copy(
            staged.at[index], sent_ref.at[0, pl.ds(0, rows)], out_sems.at[index]
        ).wait()
        return carry

    lax.fori_loop(0, found, leave, 0)
    for copy in tail_copies:
        copy.wait()


def attend_kernel(first_slot, sent_slot, tags_ref, sent_ref, after_ref, *refs):
    (
        *cache_refs, out_ref, held, staged, keys, values, even_scores, odd_scores,
        even_peak, odd_peak, at_ref, cache_ref, length_ref, in_sems, out_sems, cache_sems,
    ) = refs
    places = len(cache_refs) // 2
    sources, slots = out_ref.shape[0], out_ref.shape[2]
    rows, width = held.shape[1], held.shape[2]
    heads = width // HEAD
    parts = rows // 8
    scale = math.log2(math.e) / math.sqrt(HEAD)

    loads = []
    for place in range(places):
        for side, (whole, cached) in enumerate(
            ((keys, cache_refs[place]), (values, cache_refs[places + place]))
        ):
            loads.append(
                pltpu.make_async_copy(
                    cached, whole.at[pl.ds(place * CAPC, CAPC)], cache_sems.at[2 * place + side]
                )
            )
            loads[-1].start()

    def collect(index, found):
        slot = index // sources
        source = index - slot * sources
        row = tags_ref[source, first_slot + slot]

        @pl.when(row > 0)
        def _():
            pltpu.make_async_copy(
                sent_ref.at[
                    source, pl.ds(pl.multiple_of((slot + sent_slot) * rows, rows), rows)
                ],
                held.at[found],
                in_sems.at[found],
            ).start()
            at_ref[found] = index
            cache_ref[found] = slot // CAPC * CAPC + row - 1
            length_ref[found] = tags_ref[source, 64 + first_slot + slot]

        return found + jnp.where(row > 0, 1, 0)

    found = lax.fori_loop(0, sources * slots, collect, 0)
    for spare in range(2):
        cache_ref[found + spare] = 0
        length_ref[found + spare] = 0
    for load in loads:
        load.wait()

    def arrive(index, carry):
        pltpu.make_async_copy(sent_ref.at[0, pl.ds(0, rows)], held.at[index], in_sems.at[index]).wait()
        return carry

    lax.fori_loop(0, found, arrive, 0)

    def score(index, scores_ref, peak_ref):
        block = jnp.concatenate(
            [held[index, :, head * HEAD : (head + 1) * HEAD] for head in range(heads)], axis=0
        )
        scores = lax.dot_general(
            block, keys[cache_ref[index]], (((1,), (1,)), ((), ())),
            preferred_element_type=jnp.float32,
        )
        scores_ref[...] = scores
        peak_ref[...] = jnp.broadcast_to(jnp.max(scores, axis=1, keepdims=True), peak_ref.shape)

    def mix(index, scores_ref, peak_ref):
        peak = peak_ref[:, :1]
        weights = jnp.exp2((scores_ref[...] - peak) * scale)
        total = jnp.sum(weights, axis=1, keepdims=True)
        mixed = lax.dot_general(
            weights.astype(jnp.bfloat16), values[cache_ref[index]], (((1,), (0,)), ((), ())),
            preferred_element_type=jnp.float32,
        )
        mixed = mixed * (1.0 / total)
        line = lax.broadcasted_iota(jnp.int32, (8, HEAD), 0)
        length = length_ref[index]
        for part in range(parts):
            live = line + 8 * part < length
            for head in range(heads):
                piece = mixed[head * rows + 8 * part : head * rows + 8 * part + 8]
                staged[index, part, :, head * HEAD : (head + 1) * HEAD] = jnp.where(
                    live, piece, 0.0
                ).astype(jnp.bfloat16)

    def deliver(index):
        at = at_ref[index]
        slot = at // sources
        pltpu.make_async_copy(
            staged.at[index], out_ref.at[at - slot * sources, :, slot], out_sems.at[index]
        ).start()

    score(0, even_scores, even_peak)

    def pair(step, carry):
        first = 2 * step
        score(first + 1, odd_scores, odd_peak)
        mix(first, even_scores, even_peak)
        deliver(first)
        score(first + 2, even_scores, even_peak)
        mix(first + 1, odd_scores, odd_peak)

        @pl.when(first + 1 < found)
        def _():
            deliver(first + 1)

        return carry

    lax.fori_loop(0, (found + 1) // 2, pair, 0)

    def leave(index, carry):
        pltpu.make_async_copy(staged.at[index], out_ref.at[0, :, 0], out_sems.at[index]).wait()
        return carry

    lax.fori_loop(0, found, leave, 0)


def join_kernel(bounds, z_ref, slots_ref, prompts_ref, *refs):
    count = len(bounds) - 1
    moved_refs = refs[:count]
    out_ref, held, slot_ref, prompt_ref, counts_ref, item_ref, in_sems, out_sems, sems = refs[-9:]
    items = held.shape[0]
    columns, width = moved_refs[0].shape[1], moved_refs[0].shape[4]
    smalls = [
        pltpu.make_async_copy(slots_ref, slot_ref, sems.at[0]),
        pltpu.make_async_copy(prompts_ref, prompt_ref, sems.at[1]),
    ]
    for copy in smalls:
        copy.start()
    my_z = z_ref[0]
    for group in range(counts_ref.shape[0]):
        counts_ref[group] = 0
    for copy in smalls:
        copy.wait()

    def fetch(item, found):
        owner_x, slot, _ = route(prompt_ref[item], slot_ref, counts_ref, my_z)
        for index in range(count):
            low, high = bounds[index], bounds[index + 1]

            @pl.when((slot >= low) & (slot < high))
            def _(index=index, low=low):
                for column in range(columns):
                    pltpu.make_async_copy(
                        moved_refs[index].at[owner_x, column, slot - low],
                        held.at[found, :, pl.ds(column * width, width)],
                        in_sems.at[found],
                    ).start()
                item_ref[found] = item

        inside = (slot >= bounds[0]) & (slot < bounds[-1])
        return found + jnp.where(inside, 1, 0)

    found = lax.fori_loop(0, items, fetch, 0)

    def place(index, carry):
        pltpu.make_async_copy(out_ref.at[0], held.at[index], in_sems.at[index]).wait()
        pltpu.make_async_copy(
            held.at[index], out_ref.at[item_ref[index]], out_sems.at[index]
        ).start()
        return carry

    lax.fori_loop(0, found, place, 0)

    def leave(index, carry):
        pltpu.make_async_copy(held.at[index], out_ref.at[0], out_sems.at[index]).wait()
        return carry

    lax.fori_loop(0, found, leave, 0)


def smem():
    return pl.BlockSpec(memory_space=pltpu.SMEM)


def hbm():
    return pl.BlockSpec(memory_space=pltpu.HBM)


def attend_call(tags, sent, used, first, count, ts=8, sent_slot=0, after=None):
    xs, rows, width = sent.shape[0], 64, sent.shape[2]
    heads, prefix = width // HEAD, used[0][0].shape[1]
    return pl.pallas_call(
        functools.partial(attend_kernel, first, sent_slot),
        out_shape=jax.ShapeDtypeStruct((xs, ts, count, rows // ts, width), jnp.bfloat16),
        in_specs=[smem(), hbm(), hbm()] + [hbm()] * (2 * len(used)),
        out_specs=hbm(),
        scratch_shapes=[
            pltpu.VMEM((xs * count + 2, rows, width), jnp.bfloat16),
            pltpu.VMEM((xs * count + 1, ts, rows // ts, width), jnp.bfloat16),
            pltpu.VMEM((count, prefix, HEAD), jnp.bfloat16),
            pltpu.VMEM((count, prefix, HEAD), jnp.bfloat16),
            pltpu.VMEM((rows * heads, prefix), jnp.float32),
            pltpu.VMEM((rows * heads, prefix), jnp.float32),
            pltpu.VMEM((rows * heads, HEAD), jnp.float32),
            pltpu.VMEM((rows * heads, HEAD), jnp.float32),
            pltpu.SMEM((xs * count + 2,), jnp.int32),
            pltpu.SMEM((xs * count + 2,), jnp.int32),
            pltpu.SMEM((xs * count + 2,), jnp.int32),
            pltpu.SemaphoreType.DMA((xs * count,)),
            pltpu.SemaphoreType.DMA((xs * count,)),
            pltpu.SemaphoreType.DMA((count,)),
        ],
        compiler_params=pltpu.CompilerParams(vmem_limit_bytes=VMEM),
        cost_estimate=pl.CostEstimate(
            flops=4 * xs * count * rows * heads * prefix * HEAD,
            bytes_accessed=4 * xs * count * rows * width,
            transcendentals=xs * count * rows * heads * prefix,
        ),
    )(tags, sent, tags if after is None else after, *[c[0] for c in used], *[c[1] for c in used])


def steps(queries, prefix_keys, prefix_values, slot_of_prompt, prompt_of, lengths):
    xs, zs, ts = lax.axis_size("x"), lax.axis_size("z"), lax.axis_size("t")
    items, rows, width = queries.shape
    prefix = prefix_keys.shape[1]
    my_z = lax.axis_index("z").reshape(1)
    slot_total = zs * CAPC
    near_slots = NEAR * CAPC
    far_slots = slot_total - near_slots

    up = [(i, (i + 1) % zs) for i in range(zs)]
    down = [(i, (i - 1) % zs) for i in range(zs)]
    from_below, from_above = [(prefix_keys, prefix_values)], [(prefix_keys, prefix_values)]
    for _ in range(1, 4):
        from_below.append(tuple(lax.ppermute(a, "z", up) for a in from_below[-1]))
        from_above.append(tuple(lax.ppermute(a, "z", down) for a in from_above[-1]))
    opposite = (lax.ppermute(from_below[3][0], "z", up), lax.ppermute(from_above[3][1], "z", down))
    caches = [from_below[0]]
    for step in range(1, 4):
        caches += [from_above[step], from_below[step]]
    caches.append(opposite)

    tables = rotary_tables(prefix, rows)

    def pack(low, high, tail):
        return pl.pallas_call(
            functools.partial(pack_kernel, low, high),
            out_shape=jax.ShapeDtypeStruct(
                (xs, (high - low) * rows + tail, width), jnp.bfloat16
            ),
            in_specs=[smem()] + [hbm()] * 5,
            out_specs=hbm(),
            scratch_shapes=[
                pltpu.VMEM((items + TURN, rows, width), jnp.bfloat16),
                pltpu.VMEM((items + TURN, rows, width), jnp.bfloat16),
                pltpu.VMEM((2, rows, HEAD), jnp.float32),
                pltpu.VMEM((xs, TAIL, HEAD), jnp.bfloat16),
                pltpu.SMEM((xs * zs * CAPC,), jnp.int32),
                pltpu.SMEM((items,), jnp.int32),
                pltpu.SMEM((items,), jnp.int32),
                pltpu.SMEM((xs * zs,), jnp.int32),
                pltpu.SMEM((items,), jnp.int32),
                pltpu.SMEM((items,), jnp.int32),
                pltpu.SemaphoreType.DMA((items,)),
                pltpu.SemaphoreType.DMA((items,)),
                pltpu.SemaphoreType.DMA((4,)),
                pltpu.SemaphoreType.DMA((xs,)),
            ],
            compiler_params=pltpu.CompilerParams(vmem_limit_bytes=VMEM),
            cost_estimate=pl.CostEstimate(
                flops=2 * 10**9, bytes_accessed=items * rows * width * 2, transcendentals=0
            ),
        )(my_z, slot_of_prompt, prompt_of, lengths, queries, tables)

    near = pack(0, near_slots, TAIL)
    far = pack(near_slots, slot_total, 0)
    near = lax.all_to_all(near, "x", 0, 0, tiled=True)
    far = lax.all_to_all(far, "x", 0, 0, tiled=True)
    tags = near[:, near_slots * rows, :].astype(jnp.int32)[:, :HEAD]

    def attend(sent, first, count, sent_slot, after):
        used = caches[first // CAPC : (first + count) // CAPC]
        return attend_call(tags, sent, used, first, count, ts, sent_slot, after)

    def back(attended):
        shape = attended.shape
        moved = lax.all_to_all(
            attended.reshape(xs * ts, *shape[2:]), ("x", "t"), 0, 0, tiled=True
        )
        return moved.reshape(shape)

    near = attend(near, 0, near_slots, 0, None)
    far = attend(far, near_slots, far_slots, 0, near)
    near = back(near)
    far = back(far)

    def join(bounds, moved, out):
        more = [] if out is None else [out]
        return pl.pallas_call(
            functools.partial(join_kernel, bounds),
            out_shape=jax.ShapeDtypeStruct((items, rows // ts, width * ts), jnp.bfloat16),
            in_specs=[smem()] + [hbm()] * (2 + len(moved) + len(more)),
            out_specs=hbm(),
            input_output_aliases={3 + len(moved): 0} if more else {},
            scratch_shapes=[
                pltpu.VMEM((items, rows // ts, width * ts), jnp.bfloat16),
                pltpu.SMEM((xs * zs * CAPC,), jnp.int32),
                pltpu.SMEM((items,), jnp.int32),
                pltpu.SMEM((xs * zs,), jnp.int32),
                pltpu.SMEM((items,), jnp.int32),
                pltpu.SemaphoreType.DMA((items,)),
                pltpu.SemaphoreType.DMA((items,)),
                pltpu.SemaphoreType.DMA((2,)),
            ],
            compiler_params=pltpu.CompilerParams(vmem_limit_bytes=VMEM),
            cost_estimate=pl.CostEstimate(
                flops=10**9, bytes_accessed=2 * items * rows * width, transcendentals=0
            ),
        )(my_z, slot_of_prompt, prompt_of, *moved, *more)

    out = join((0, near_slots), [near], None)
    return join((near_slots, slot_total), [far], out)


def solution(mesh):
    groups, tensors = mesh.devices.shape
    grid = Mesh(
        mesh.devices.reshape(groups // GROUPS_Z, GROUPS_Z, tensors), ("x", "z", "t")
    )
    split = P(("x", "z"), None, "t")
    return jax.shard_map(
        steps,
        mesh=grid,
        in_specs=(split, split, split, P(), P(("x", "z")), P(("x", "z"))),
        out_specs=P(("x", "z"), "t", None),
        check_vma=False,
    )
```

```python
import functools
import math

import jax
import jax.numpy as jnp
import numpy as np
from jax import lax
from jax.experimental import pallas as pl
from jax.experimental.pallas import tpu as pltpu
from jax.sharding import Mesh, PartitionSpec as P


HEAD = 128
CAPC = 2
ROTARY_BASE = 1000000.0
VMEM = 67043328
GROUPS_Z = 8
THERE = (0, 3 * CAPC, 8 * CAPC)
BOUNDS = (0, 3 * CAPC, 5 * CAPC, 8 * CAPC)
TURN = 4


def rotary_tables(first_position, rows):
    half = HEAD // 2
    frequencies = np.float32(ROTARY_BASE) ** (
        -(np.arange(half, dtype=np.float32) * np.float32(2.0) / np.float32(HEAD))
    )
    positions = np.arange(first_position, first_position + rows).astype(np.float32)
    angles = (positions[:, None] * frequencies[None, :]).astype(np.float32).astype(np.float64)
    cos, sin = np.cos(angles), np.sin(angles)
    return np.stack(
        [np.concatenate([cos, cos], axis=1), np.concatenate([-sin, sin], axis=1)]
    ).astype(np.float32)


def route(prompt, slot_ref, counts_ref, my_z):
    cache_slot = slot_ref[prompt]
    owner = cache_slot // 2
    row = cache_slot - owner * 2
    owner_x = owner // GROUPS_Z
    distance = lax.rem(owner - owner_x * GROUPS_Z - my_z + GROUPS_Z, GROUPS_Z)
    place = jnp.where(
        distance == 0, 0, jnp.where(distance <= 4, 2 * distance - 1, 2 * (GROUPS_Z - distance))
    )
    arrival = counts_ref[owner]
    counts_ref[owner] = arrival + 1
    return owner_x, place * CAPC + arrival, row


def pack_kernel(
    xs, x_ref, z_ref, slots_ref, prompts_ref, lengths_ref, queries_ref, tables_ref, *refs
):
    sent_refs, tag_ref = refs[:-11], refs[-11]
    (
        held, staged, tables, slot_ref, prompt_ref, length_ref, counts_ref,
        in_sems, out_sems, small_sems,
    ) = refs[-10:]
    items, rows, width = queries_ref.shape
    heads = width // HEAD
    my_x, my_z = x_ref[0], z_ref[0]
    smalls = [
        pltpu.make_async_copy(source, target, small_sems.at[index])
        for index, (source, target) in enumerate(
            (
                (slots_ref, slot_ref), (prompts_ref, prompt_ref), (lengths_ref, length_ref),
                (tables_ref, tables),
            )
        )
    ]
    for copy in smalls:
        copy.start()
    for item in range(items):
        pltpu.make_async_copy(queries_ref.at[item], held.at[item], in_sems.at[item]).start()
    for group in range(counts_ref.shape[0]):
        counts_ref[group] = 0
    line = lax.broadcasted_iota(jnp.int32, (8, HEAD), 0)
    lane = lax.broadcasted_iota(jnp.int32, (8, HEAD), 1)
    for copy in smalls:
        copy.wait()

    def turn(step, tags):
        for inner in range(TURN):
            item = step * TURN + inner
            pltpu.make_async_copy(queries_ref.at[item], held.at[item], in_sems.at[item]).wait()
        routes = []
        for inner in range(TURN):
            item = step * TURN + inner
            owner_x, slot, row = route(prompt_ref[item], slot_ref, counts_ref, my_z)
            routes.append((item, lax.rem(owner_x - my_x + xs, xs), slot))
            tags = jnp.where((line == owner_x) & (lane == slot), row + 1, tags)
            tags = jnp.where((line == owner_x) & (lane == slot + 64), length_ref[item], tags)
            for head in range(heads):
                part = held[item, :, head * HEAD : (head + 1) * HEAD].astype(jnp.float32)
                turned = part * tables[0] + pltpu.roll(part, HEAD // 2, 1) * tables[1]
                staged[item, :, head * HEAD : (head + 1) * HEAD] = turned.astype(jnp.bfloat16)
        for item, shift, slot in routes:
            for index, sent_ref in enumerate(sent_refs):
                low, high = THERE[index // xs], THERE[index // xs + 1]

                @pl.when((shift == index % xs) & (slot >= low) & (slot < high))
                def _(item=item, slot=slot, low=low, sent_ref=sent_ref):
                    at = pl.ds(pl.multiple_of((slot - low) * rows, rows), rows)
                    pltpu.make_async_copy(
                        staged.at[item], sent_ref.at[at], out_sems.at[item]
                    ).start()

        return tags

    none = jnp.zeros((8, HEAD), jnp.int32)
    tag_ref[...] = lax.fori_loop(0, items // TURN, turn, none)[:xs]
    for item in range(items):
        pltpu.make_async_copy(
            staged.at[item], sent_refs[0].at[pl.ds(0, rows)], out_sems.at[item]
        ).wait()


def attend_kernel(first_slot, skip, xs, x_ref, tags_ref, *refs):
    sent_refs = refs[:xs]
    (
        *cache_refs, out_ref, held, staged, keys, values, even_scores, odd_scores,
        even_peak, odd_peak, at_ref, cache_ref, length_ref, in_sems, out_sems, cache_sems,
    ) = refs[xs + 1 :]
    places = len(cache_refs) // 2
    my_x = x_ref[0]
    sources, slots = out_ref.shape[1], out_ref.shape[2]
    rows, width = held.shape[1], held.shape[2]
    heads = width // HEAD
    parts = rows // 8
    scale = math.log2(math.e) / math.sqrt(HEAD)

    loads = []
    for place in range(places):
        for side, (whole, cached) in enumerate(
            ((keys, cache_refs[place]), (values, cache_refs[places + place]))
        ):
            loads.append(
                pltpu.make_async_copy(
                    cached, whole.at[pl.ds(place * CAPC, CAPC)], cache_sems.at[2 * place + side]
                )
            )
            loads[-1].start()

    def collect(slot, found):
        for shift in range(xs):
            source = lax.rem(my_x - shift + xs, xs)
            row = tags_ref[source, first_slot + slot]

            @pl.when(row > 0)
            def _(shift=shift, source=source, row=row, found=found):
                pltpu.make_async_copy(
                    sent_refs[shift].at[pl.ds(pl.multiple_of((slot + skip) * rows, rows), rows)],
                    held.at[found],
                    in_sems.at[found],
                ).start()
                at_ref[found] = slot * sources + source
                cache_ref[found] = slot // CAPC * CAPC + row - 1
                length_ref[found] = tags_ref[source, 64 + first_slot + slot]

            found = found + jnp.where(row > 0, 1, 0)
        return found

    found = lax.fori_loop(0, slots, collect, 0)
    for spare in range(2):
        cache_ref[found + spare] = 0
        length_ref[found + spare] = 0
    for load in loads:
        load.wait()

    def arrive(index, carry):
        pltpu.make_async_copy(
            sent_refs[0].at[pl.ds(0, rows)], held.at[index], in_sems.at[index]
        ).wait()
        return carry

    lax.fori_loop(0, found, arrive, 0)

    def score(index, scores_ref, peak_ref):
        block = jnp.concatenate(
            [held[index, :, head * HEAD : (head + 1) * HEAD] for head in range(heads)], axis=0
        )
        scores = lax.dot_general(
            block, keys[cache_ref[index]], (((1,), (1,)), ((), ())),
            preferred_element_type=jnp.float32,
        )
        scores_ref[...] = scores
        peak_ref[...] = jnp.broadcast_to(jnp.max(scores, axis=1, keepdims=True), peak_ref.shape)

    def mix(index, scores_ref, peak_ref):
        peak = peak_ref[:, :1]
        weights = jnp.exp2((scores_ref[...] - peak) * scale)
        total = jnp.sum(weights, axis=1, keepdims=True)
        mixed = lax.dot_general(
            weights.astype(jnp.bfloat16), values[cache_ref[index]], (((1,), (0,)), ((), ())),
            preferred_element_type=jnp.float32,
        )
        mixed = mixed * (1.0 / total)
        line = lax.broadcasted_iota(jnp.int32, (8, HEAD), 0)
        length = length_ref[index]
        for part in range(parts):
            live = line + 8 * part < length
            for head in range(heads):
                piece = mixed[head * rows + 8 * part : head * rows + 8 * part + 8]
                staged[index, part, :, head * HEAD : (head + 1) * HEAD] = jnp.where(
                    live, piece, 0.0
                ).astype(jnp.bfloat16)

    def deliver(index):
        at = at_ref[index]
        slot = at // sources
        pltpu.make_async_copy(
            staged.at[index], out_ref.at[:, at - slot * sources, slot], out_sems.at[index]
        ).start()

    score(0, even_scores, even_peak)

    def pair(step, carry):
        first = 2 * step
        score(first + 1, odd_scores, odd_peak)
        mix(first, even_scores, even_peak)
        deliver(first)
        score(first + 2, even_scores, even_peak)
        mix(first + 1, odd_scores, odd_peak)

        @pl.when(first + 1 < found)
        def _():
            deliver(first + 1)

        return carry

    lax.fori_loop(0, (found + 1) // 2, pair, 0)

    def leave(index, carry):
        pltpu.make_async_copy(staged.at[index], out_ref.at[:, 0, 0], out_sems.at[index]).wait()
        return carry

    lax.fori_loop(0, found, leave, 0)


def join_kernel(bounds, z_ref, slots_ref, prompts_ref, *refs):
    count = len(bounds) - 1
    moved_refs = refs[:count]
    out_ref, held, slot_ref, prompt_ref, counts_ref, item_ref, in_sems, out_sems, sems = refs[-9:]
    items = held.shape[0]
    columns, width = moved_refs[0].shape[0], moved_refs[0].shape[4]
    smalls = [
        pltpu.make_async_copy(slots_ref, slot_ref, sems.at[0]),
        pltpu.make_async_copy(prompts_ref, prompt_ref, sems.at[1]),
    ]
    for copy in smalls:
        copy.start()
    my_z = z_ref[0]
    for group in range(counts_ref.shape[0]):
        counts_ref[group] = 0
    for copy in smalls:
        copy.wait()

    def fetch(item, found):
        owner_x, slot, _ = route(prompt_ref[item], slot_ref, counts_ref, my_z)
        for index in range(count):
            low, high = bounds[index], bounds[index + 1]

            @pl.when((slot >= low) & (slot < high))
            def _(index=index, low=low):
                for column in range(columns):
                    pltpu.make_async_copy(
                        moved_refs[index].at[column, owner_x, slot - low],
                        held.at[found, :, pl.ds(column * width, width)],
                        in_sems.at[found],
                    ).start()
                item_ref[found] = item

        inside = (slot >= bounds[0]) & (slot < bounds[-1])
        return found + jnp.where(inside, 1, 0)

    found = lax.fori_loop(0, items, fetch, 0)

    def place(index, carry):
        pltpu.make_async_copy(out_ref.at[0], held.at[index], in_sems.at[index]).wait()
        pltpu.make_async_copy(
            held.at[index], out_ref.at[item_ref[index]], out_sems.at[index]
        ).start()
        return carry

    lax.fori_loop(0, found, place, 0)

    def leave(index, carry):
        pltpu.make_async_copy(held.at[index], out_ref.at[0], out_sems.at[index]).wait()
        return carry

    lax.fori_loop(0, found, leave, 0)


def smem():
    return pl.BlockSpec(memory_space=pltpu.SMEM)


def vmem():
    return pl.BlockSpec(memory_space=pltpu.VMEM)


def hbm():
    return pl.BlockSpec(memory_space=pltpu.HBM)


def attend_call(my_x, tags, sent, used, first, skip, count, rows, ts, after):
    xs, width = len(sent), sent[0].shape[1]
    heads, prefix = width // HEAD, used[0][0].shape[1]
    return pl.pallas_call(
        functools.partial(attend_kernel, first, skip, xs),
        out_shape=jax.ShapeDtypeStruct((ts, xs, count, rows // ts, width), jnp.bfloat16),
        in_specs=[smem(), smem()] + [hbm()] * (xs + 1 + 2 * len(used)),
        out_specs=hbm(),
        scratch_shapes=[
            pltpu.VMEM((xs * count + 2, rows, width), jnp.bfloat16),
            pltpu.VMEM((xs * count + 1, ts, rows // ts, width), jnp.bfloat16),
            pltpu.VMEM((count, prefix, HEAD), jnp.bfloat16),
            pltpu.VMEM((count, prefix, HEAD), jnp.bfloat16),
            pltpu.VMEM((rows * heads, prefix), jnp.float32),
            pltpu.VMEM((rows * heads, prefix), jnp.float32),
            pltpu.VMEM((rows * heads, HEAD), jnp.float32),
            pltpu.VMEM((rows * heads, HEAD), jnp.float32),
            pltpu.SMEM((xs * count + 2,), jnp.int32),
            pltpu.SMEM((xs * count + 2,), jnp.int32),
            pltpu.SMEM((xs * count + 2,), jnp.int32),
            pltpu.SemaphoreType.DMA((xs * count,)),
            pltpu.SemaphoreType.DMA((xs * count,)),
            pltpu.SemaphoreType.DMA((count,)),
        ],
        compiler_params=pltpu.CompilerParams(vmem_limit_bytes=VMEM),
        cost_estimate=pl.CostEstimate(
            flops=4 * xs * count * rows * heads * prefix * HEAD,
            bytes_accessed=4 * xs * count * rows * width,
            transcendentals=xs * count * rows * heads * prefix,
        ),
    )(my_x, tags, *sent, after, *[c[0] for c in used], *[c[1] for c in used])


def steps(queries, prefix_keys, prefix_values, slot_of_prompt, prompt_of, lengths):
    xs, zs, ts = lax.axis_size("x"), lax.axis_size("z"), lax.axis_size("t")
    items, rows, width = queries.shape
    prefix = prefix_keys.shape[1]
    my_x, my_z = lax.axis_index("x").reshape(1), lax.axis_index("z").reshape(1)

    up = [(i, (i + 1) % zs) for i in range(zs)]
    down = [(i, (i - 1) % zs) for i in range(zs)]
    from_below, from_above = [(prefix_keys, prefix_values)], [(prefix_keys, prefix_values)]
    for _ in range(1, 4):
        from_below.append(tuple(lax.ppermute(a, "z", up) for a in from_below[-1]))
        from_above.append(tuple(lax.ppermute(a, "z", down) for a in from_above[-1]))
    opposite = (lax.ppermute(from_below[3][0], "z", up), lax.ppermute(from_above[3][1], "z", down))
    caches = [from_below[0]]
    for step in range(1, 4):
        caches += [from_above[step], from_below[step]]
    caches.append(opposite)

    *packed, tags = pl.pallas_call(
        functools.partial(pack_kernel, xs),
        out_shape=[
            jax.ShapeDtypeStruct(((high - low) * rows, width), jnp.bfloat16)
            for low, high in zip(THERE[:-1], THERE[1:])
            for _ in range(xs)
        ]
        + [jax.ShapeDtypeStruct((xs, HEAD), jnp.int32)],
        in_specs=[smem()] * 2 + [hbm()] * 5,
        out_specs=[hbm()] * (xs * (len(THERE) - 1)) + [vmem()],
        scratch_shapes=[
            pltpu.VMEM((items, rows, width), jnp.bfloat16),
            pltpu.VMEM((items, rows, width), jnp.bfloat16),
            pltpu.VMEM((2, rows, HEAD), jnp.float32),
            pltpu.SMEM((xs * zs * CAPC,), jnp.int32),
            pltpu.SMEM((items,), jnp.int32),
            pltpu.SMEM((items,), jnp.int32),
            pltpu.SMEM((xs * zs,), jnp.int32),
            pltpu.SemaphoreType.DMA((items,)),
            pltpu.SemaphoreType.DMA((items,)),
            pltpu.SemaphoreType.DMA((4,)),
        ],
        compiler_params=pltpu.CompilerParams(vmem_limit_bytes=VMEM),
        cost_estimate=pl.CostEstimate(
            flops=4 * 10**9, bytes_accessed=2 * items * rows * width * 2, transcendentals=0
        ),
    )(my_x, my_z, slot_of_prompt, prompt_of, lengths, queries, rotary_tables(prefix, rows))

    def there(sent):
        return [sent[0]] + [
            lax.ppermute(sent[k], "x", [(i, (i + k) % xs) for i in range(xs)])
            for k in range(1, xs)
        ]

    sent = []
    for index in range(len(THERE) - 1):
        sent.append(there(packed[index * xs : (index + 1) * xs]))
    tags = lax.all_to_all(tags, "x", 0, 0, tiled=True)

    def attend(first, count, after):
        used = caches[first // CAPC : (first + count) // CAPC]
        part = sum(first >= low for low in THERE[1:])
        return attend_call(
            my_x, tags, sent[part], used, first, first - THERE[part], count, rows, ts, after
        )

    def back(attended):
        shape = attended.shape
        moved = lax.all_to_all(
            attended.reshape(ts * xs, *shape[2:]), ("t", "x"), 0, 0, tiled=True
        )
        return moved.reshape(shape)

    moved, after = [], tags
    for low, high in zip(BOUNDS[:-1], BOUNDS[1:]):
        after = attend(low, high - low, after)
        moved.append(back(after))

    def join(bounds, moved, out):
        more = [] if out is None else [out]
        return pl.pallas_call(
            functools.partial(join_kernel, bounds),
            out_shape=jax.ShapeDtypeStruct((items, rows // ts, width * ts), jnp.bfloat16),
            in_specs=[smem()] + [hbm()] * (2 + len(moved) + len(more)),
            out_specs=hbm(),
            input_output_aliases={3 + len(moved): 0} if more else {},
            scratch_shapes=[
                pltpu.VMEM((items, rows // ts, width * ts), jnp.bfloat16),
                pltpu.SMEM((xs * zs * CAPC,), jnp.int32),
                pltpu.SMEM((items,), jnp.int32),
                pltpu.SMEM((xs * zs,), jnp.int32),
                pltpu.SMEM((items,), jnp.int32),
                pltpu.SemaphoreType.DMA((items,)),
                pltpu.SemaphoreType.DMA((items,)),
                pltpu.SemaphoreType.DMA((2,)),
            ],
            compiler_params=pltpu.CompilerParams(vmem_limit_bytes=VMEM),
            cost_estimate=pl.CostEstimate(
                flops=10**9, bytes_accessed=2 * items * rows * width, transcendentals=0
            ),
        )(my_z, slot_of_prompt, prompt_of, *moved, *more)

    out = join(BOUNDS[:-1], moved[:-1], None)
    return join(BOUNDS[-2:], moved[-1:], out)


def solution(mesh):
    groups, tensors = mesh.devices.shape
    grid = Mesh(
        mesh.devices.reshape(groups // GROUPS_Z, GROUPS_Z, tensors), ("x", "z", "t")
    )
    split = P(("x", "z"), None, "t")
    return jax.shard_map(
        steps,
        mesh=grid,
        in_specs=(split, split, split, P(), P(("x", "z")), P(("x", "z"))),
        out_specs=P(("x", "z"), "t", None),
        check_vma=False,
    )
```

```python
import functools
import math

import jax
import jax.numpy as jnp
import numpy as np
from jax import lax
from jax.experimental import pallas as pl
from jax.experimental.pallas import tpu as pltpu
from jax.sharding import Mesh, PartitionSpec as P


HEAD = 128
CAPC = 2
ROTARY_BASE = 1000000.0
VMEM = 67043328
GROUPS_Z = 8
THERE = (0, 3 * CAPC, 7 * CAPC, 8 * CAPC)
BOUNDS = (0, 3 * CAPC, 5 * CAPC, 8 * CAPC)
ATTEND = (0, CAPC, 3 * CAPC, 5 * CAPC, 7 * CAPC, 8 * CAPC)
TURN = 4


def rotary_tables(first_position, rows):
    half = HEAD // 2
    frequencies = np.float32(ROTARY_BASE) ** (
        -(np.arange(half, dtype=np.float32) * np.float32(2.0) / np.float32(HEAD))
    )
    positions = np.arange(first_position, first_position + rows).astype(np.float32)
    angles = (positions[:, None] * frequencies[None, :]).astype(np.float32).astype(np.float64)
    cos, sin = np.cos(angles), np.sin(angles)
    return np.stack(
        [np.concatenate([cos, cos], axis=1), np.concatenate([-sin, sin], axis=1)]
    ).astype(np.float32)


def route(prompt, slot_ref, counts_ref, my_z):
    cache_slot = slot_ref[prompt]
    owner = cache_slot // 2
    row = cache_slot - owner * 2
    owner_x = owner // GROUPS_Z
    distance = lax.rem(owner - owner_x * GROUPS_Z - my_z + GROUPS_Z, GROUPS_Z)
    place = jnp.where(
        distance == 0, 0, jnp.where(distance <= 4, 2 * distance - 1, 2 * (GROUPS_Z - distance))
    )
    arrival = counts_ref[owner]
    counts_ref[owner] = arrival + 1
    return owner_x, place * CAPC + arrival, row


def choose(value, low, high, act):
    if high - low == 1:
        act(low)
        return
    middle = (low + high) // 2
    lax.cond(
        value < middle,
        lambda: choose(value, low, middle, act),
        lambda: choose(value, middle, high, act),
    )


def pack_kernel(xs, x_ref, z_ref, slots_ref, prompts_ref, lengths_ref, queries_ref, *refs):
    sent_refs, tag_ref = refs[:-9], refs[-9]
    held, slot_ref, prompt_ref, length_ref, counts_ref, in_sems, out_sems, small_sems = refs[-8:]
    items, rows, _ = queries_ref.shape
    my_x, my_z = x_ref[0], z_ref[0]
    smalls = [
        pltpu.make_async_copy(source, target, small_sems.at[index])
        for index, (source, target) in enumerate(
            ((slots_ref, slot_ref), (prompts_ref, prompt_ref), (lengths_ref, length_ref))
        )
    ]
    for copy in smalls:
        copy.start()
    for item in range(items):
        pltpu.make_async_copy(queries_ref.at[item], held.at[item], in_sems.at[item]).start()
    for group in range(counts_ref.shape[0]):
        counts_ref[group] = 0
    line = lax.broadcasted_iota(jnp.int32, (8, HEAD), 0)
    lane = lax.broadcasted_iota(jnp.int32, (8, HEAD), 1)
    for copy in smalls:
        copy.wait()

    def turn(step, tags):
        routes = []
        for inner in range(TURN):
            item = step * TURN + inner
            owner_x, slot, row = route(prompt_ref[item], slot_ref, counts_ref, my_z)
            routes.append((item, lax.rem(owner_x - my_x + xs, xs), slot))
            tags = jnp.where((line == owner_x) & (lane == slot), row + 1, tags)
            tags = jnp.where((line == owner_x) & (lane == slot + 64), length_ref[item], tags)
        for item, shift, slot in routes:
            part = sum((slot >= low).astype(jnp.int32) for low in THERE[1:-1])
            pltpu.make_async_copy(queries_ref.at[item], held.at[item], in_sems.at[item]).wait()

            def start(index, item=item, slot=slot):
                at = pl.ds(pl.multiple_of((slot - THERE[index // xs]) * rows, rows), rows)
                pltpu.make_async_copy(
                    held.at[item], sent_refs[index].at[at], out_sems.at[item]
                ).start()

            choose(part * xs + shift, 0, len(sent_refs), start)
        return tags

    none = jnp.zeros((8, HEAD), jnp.int32)
    tag_ref[...] = lax.fori_loop(0, items // TURN, turn, none)[:xs]
    for item in range(items):
        pltpu.make_async_copy(
            held.at[item], sent_refs[0].at[pl.ds(0, rows)], out_sems.at[item]
        ).wait()


def attend_kernel(first_slot, slots, skip, out_skip, xs, x_ref, tags_ref, tables_ref, *refs):
    sent_refs = refs[:xs]
    (
        *cache_refs, out_ref, held, staged, keys, values, even_scores, odd_scores,
        even_peak, odd_peak, tables, at_ref, cache_ref, length_ref, in_sems, out_sems, cache_sems,
    ) = refs[xs + 1 :]
    places = len(cache_refs) // 2
    my_x = x_ref[0]
    sources = out_ref.shape[1]
    rows, width = held.shape[1], held.shape[2]
    heads = width // HEAD
    parts = rows // 8
    scale = math.log2(math.e) / math.sqrt(HEAD)

    loads = [pltpu.make_async_copy(tables_ref, tables, cache_sems.at[2 * places])]
    loads[0].start()
    for place in range(places):
        for side, (whole, cached) in enumerate(
            ((keys, cache_refs[place]), (values, cache_refs[places + place]))
        ):
            loads.append(
                pltpu.make_async_copy(
                    cached, whole.at[pl.ds(place * CAPC, CAPC)], cache_sems.at[2 * place + side]
                )
            )
            loads[-1].start()

    def collect(slot, found):
        for shift in range(xs):
            source = lax.rem(my_x - shift + xs, xs)
            row = tags_ref[source, first_slot + slot]

            @pl.when(row > 0)
            def _(shift=shift, source=source, row=row, found=found):
                pltpu.make_async_copy(
                    sent_refs[shift].at[pl.ds(pl.multiple_of((slot + skip) * rows, rows), rows)],
                    held.at[found],
                    in_sems.at[found],
                ).start()
                at_ref[found] = slot * sources + source
                cache_ref[found] = slot // CAPC * CAPC + row - 1
                length_ref[found] = tags_ref[source, 64 + first_slot + slot]

            found = found + jnp.where(row > 0, 1, 0)
        return found

    found = lax.fori_loop(0, slots, collect, 0)
    for spare in range(2):
        cache_ref[found + spare] = 0
        length_ref[found + spare] = 0
    for load in loads:
        load.wait()

    def arrive(index, carry):
        pltpu.make_async_copy(
            sent_refs[0].at[pl.ds(0, rows)], held.at[index], in_sems.at[index]
        ).wait()
        return carry

    lax.fori_loop(0, found, arrive, 0)

    def score(index, scores_ref, peak_ref):
        turned = []
        for head in range(heads):
            part = held[index, :, head * HEAD : (head + 1) * HEAD].astype(jnp.float32)
            part = part * tables[0] + pltpu.roll(part, HEAD // 2, 1) * tables[1]
            turned.append(part.astype(jnp.bfloat16))
        block = jnp.concatenate(turned, axis=0)
        scores = lax.dot_general(
            block, keys[cache_ref[index]], (((1,), (1,)), ((), ())),
            preferred_element_type=jnp.float32,
        )
        scores_ref[...] = scores
        peak_ref[...] = jnp.broadcast_to(jnp.max(scores, axis=1, keepdims=True), peak_ref.shape)

    def mix(index, scores_ref, peak_ref):
        peak = peak_ref[:, :1]
        weights = jnp.exp2((scores_ref[...] - peak) * scale)
        total = jnp.sum(weights, axis=1, keepdims=True)
        mixed = lax.dot_general(
            weights.astype(jnp.bfloat16), values[cache_ref[index]], (((1,), (0,)), ((), ())),
            preferred_element_type=jnp.float32,
        )
        mixed = mixed * (1.0 / total)
        line = lax.broadcasted_iota(jnp.int32, (8, HEAD), 0)
        length = length_ref[index]
        for part in range(parts):
            live = line + 8 * part < length
            for head in range(heads):
                piece = mixed[head * rows + 8 * part : head * rows + 8 * part + 8]
                staged[index, part, :, head * HEAD : (head + 1) * HEAD] = jnp.where(
                    live, piece, 0.0
                ).astype(jnp.bfloat16)

    def deliver(index):
        at = at_ref[index]
        slot = at // sources
        pltpu.make_async_copy(
            staged.at[index], out_ref.at[:, at - slot * sources, slot + out_skip],
            out_sems.at[index],
        ).start()

    score(0, even_scores, even_peak)

    def pair(step, carry):
        first = 2 * step
        score(first + 1, odd_scores, odd_peak)
        mix(first, even_scores, even_peak)
        deliver(first)
        score(first + 2, even_scores, even_peak)
        mix(first + 1, odd_scores, odd_peak)

        @pl.when(first + 1 < found)
        def _():
            deliver(first + 1)

        return carry

    lax.fori_loop(0, (found + 1) // 2, pair, 0)

    def leave(index, carry):
        pltpu.make_async_copy(staged.at[index], out_ref.at[:, 0, 0], out_sems.at[index]).wait()
        return carry

    lax.fori_loop(0, found, leave, 0)


def join_kernel(bounds, z_ref, slots_ref, prompts_ref, *refs):
    count = len(bounds) - 1
    moved_refs = refs[:count]
    (
        out_ref, held, joined, slot_ref, prompt_ref, counts_ref, item_ref, in_sems, out_sems, sems,
    ) = refs[-10:]
    items = held.shape[0]
    columns, width = moved_refs[0].shape[0], moved_refs[0].shape[4]
    smalls = [
        pltpu.make_async_copy(slots_ref, slot_ref, sems.at[0]),
        pltpu.make_async_copy(prompts_ref, prompt_ref, sems.at[1]),
    ]
    for copy in smalls:
        copy.start()
    my_z = z_ref[0]
    for group in range(counts_ref.shape[0]):
        counts_ref[group] = 0
    for copy in smalls:
        copy.wait()

    def fetch(item, found):
        owner_x, slot, _ = route(prompt_ref[item], slot_ref, counts_ref, my_z)
        for index in range(count):
            low, high = bounds[index], bounds[index + 1]

            @pl.when((slot >= low) & (slot < high))
            def _(index=index, low=low):
                pltpu.make_async_copy(
                    moved_refs[index].at[:, owner_x, slot - low], held.at[found], in_sems.at[found]
                ).start()
                item_ref[found] = item

        inside = (slot >= bounds[0]) & (slot < bounds[-1])
        return found + jnp.where(inside, 1, 0)

    found = lax.fori_loop(0, items, fetch, 0)

    def place(index, carry):
        pltpu.make_async_copy(
            moved_refs[0].at[:, 0, 0], held.at[index], in_sems.at[index]
        ).wait()
        for column in range(columns):
            joined[index, :, column * width : (column + 1) * width] = held[index, column]
        pltpu.make_async_copy(
            joined.at[index], out_ref.at[item_ref[index]], out_sems.at[index]
        ).start()
        return carry

    lax.fori_loop(0, found, place, 0)

    def leave(index, carry):
        pltpu.make_async_copy(joined.at[index], out_ref.at[0], out_sems.at[index]).wait()
        return carry

    lax.fori_loop(0, found, leave, 0)


def smem():
    return pl.BlockSpec(memory_space=pltpu.SMEM)


def vmem():
    return pl.BlockSpec(memory_space=pltpu.VMEM)


def hbm():
    return pl.BlockSpec(memory_space=pltpu.HBM)


def attend_call(my_x, tags, tables, sent, used, first, count, skip, out_skip, out_slots, rows, ts, after):
    xs, width = len(sent), sent[0].shape[1]
    heads, prefix = width // HEAD, used[0][0].shape[1]
    return pl.pallas_call(
        functools.partial(attend_kernel, first, count, skip, out_skip, xs),
        out_shape=jax.ShapeDtypeStruct((ts, xs, out_slots, rows // ts, width), jnp.bfloat16),
        in_specs=[smem(), smem()] + [hbm()] * (xs + 2 + 2 * len(used)),
        out_specs=hbm(),
        input_output_aliases={3 + xs: 0} if out_skip else {},
        scratch_shapes=[
            pltpu.VMEM((xs * count + 2, rows, width), jnp.bfloat16),
            pltpu.VMEM((xs * count + 1, ts, rows // ts, width), jnp.bfloat16),
            pltpu.VMEM((count, prefix, HEAD), jnp.bfloat16),
            pltpu.VMEM((count, prefix, HEAD), jnp.bfloat16),
            pltpu.VMEM((rows * heads, prefix), jnp.float32),
            pltpu.VMEM((rows * heads, prefix), jnp.float32),
            pltpu.VMEM((rows * heads, HEAD), jnp.float32),
            pltpu.VMEM((rows * heads, HEAD), jnp.float32),
            pltpu.VMEM((2, rows, HEAD), jnp.float32),
            pltpu.SMEM((xs * count + 2,), jnp.int32),
            pltpu.SMEM((xs * count + 2,), jnp.int32),
            pltpu.SMEM((xs * count + 2,), jnp.int32),
            pltpu.SemaphoreType.DMA((xs * count,)),
            pltpu.SemaphoreType.DMA((xs * count,)),
            pltpu.SemaphoreType.DMA((count + 1,)),
        ],
        compiler_params=pltpu.CompilerParams(vmem_limit_bytes=VMEM),
        cost_estimate=pl.CostEstimate(
            flops=4 * xs * count * rows * heads * prefix * HEAD,
            bytes_accessed=4 * xs * count * rows * width,
            transcendentals=xs * count * rows * heads * prefix,
        ),
    )(my_x, tags, tables, *sent, after, *[c[0] for c in used], *[c[1] for c in used])


def steps(queries, prefix_keys, prefix_values, slot_of_prompt, prompt_of, lengths):
    xs, zs, ts = lax.axis_size("x"), lax.axis_size("z"), lax.axis_size("t")
    items, rows, width = queries.shape
    prefix = prefix_keys.shape[1]
    my_x, my_z = lax.axis_index("x").reshape(1), lax.axis_index("z").reshape(1)

    up = [(i, (i + 1) % zs) for i in range(zs)]
    down = [(i, (i - 1) % zs) for i in range(zs)]
    from_below, from_above = [(prefix_keys, prefix_values)], [(prefix_keys, prefix_values)]
    for _ in range(1, 4):
        from_below.append(tuple(lax.ppermute(a, "z", up) for a in from_below[-1]))
        from_above.append(tuple(lax.ppermute(a, "z", down) for a in from_above[-1]))
    opposite = (lax.ppermute(from_below[3][0], "z", up), lax.ppermute(from_above[3][1], "z", down))
    caches = [from_below[0]]
    for step in range(1, 4):
        caches += [from_above[step], from_below[step]]
    caches.append(opposite)

    *packed, tags = pl.pallas_call(
        functools.partial(pack_kernel, xs),
        out_shape=[
            jax.ShapeDtypeStruct(((high - low) * rows, width), jnp.bfloat16)
            for low, high in zip(THERE[:-1], THERE[1:])
            for _ in range(xs)
        ]
        + [jax.ShapeDtypeStruct((xs, HEAD), jnp.int32)],
        in_specs=[smem()] * 2 + [hbm()] * 4,
        out_specs=[hbm()] * (xs * (len(THERE) - 1)) + [vmem()],
        scratch_shapes=[
            pltpu.VMEM((items, rows, width), jnp.bfloat16),
            pltpu.SMEM((xs * zs * CAPC,), jnp.int32),
            pltpu.SMEM((items,), jnp.int32),
            pltpu.SMEM((items,), jnp.int32),
            pltpu.SMEM((xs * zs,), jnp.int32),
            pltpu.SemaphoreType.DMA((items,)),
            pltpu.SemaphoreType.DMA((items,)),
            pltpu.SemaphoreType.DMA((3,)),
        ],
        compiler_params=pltpu.CompilerParams(vmem_limit_bytes=VMEM),
        cost_estimate=pl.CostEstimate(
            flops=4 * 10**9, bytes_accessed=2 * items * rows * width * 2, transcendentals=0
        ),
    )(my_x, my_z, slot_of_prompt, prompt_of, lengths, queries)
    tables = rotary_tables(prefix, rows)

    def there(sent):
        return [sent[0]] + [
            lax.ppermute(sent[k], "x", [(i, (i + k) % xs) for i in range(xs)])
            for k in range(1, xs)
        ]

    sent = []
    for index in range(len(THERE) - 1):
        sent.append(there(packed[index * xs : (index + 1) * xs]))
    tags = lax.all_to_all(tags, "x", 0, 0, tiled=True)

    def attend(first, count, after):
        used = caches[first // CAPC : (first + count) // CAPC]
        part = sum(first >= low for low in THERE[1:])
        turn = sum(first >= low for low in BOUNDS[1:])
        return attend_call(
            my_x, tags, tables, sent[part], used, first, count, first - THERE[part],
            first - BOUNDS[turn], BOUNDS[turn + 1] - BOUNDS[turn], rows, ts, after,
        )

    def back(attended):
        shape = attended.shape
        moved = lax.all_to_all(
            attended.reshape(ts * xs, *shape[2:]), ("t", "x"), 0, 0, tiled=True
        )
        return moved.reshape(shape)

    moved, after = [], tags
    for low, high in zip(ATTEND[:-1], ATTEND[1:]):
        after = attend(low, high - low, after)
        if high in BOUNDS:
            moved.append(back(after))

    def join(bounds, moved, out):
        more = [] if out is None else [out]
        return pl.pallas_call(
            functools.partial(join_kernel, bounds),
            out_shape=jax.ShapeDtypeStruct((items, rows // ts, width * ts), jnp.bfloat16),
            in_specs=[smem()] + [hbm()] * (2 + len(moved) + len(more)),
            out_specs=hbm(),
            input_output_aliases={3 + len(moved): 0} if more else {},
            scratch_shapes=[
                pltpu.VMEM((items, ts, rows // ts, width), jnp.bfloat16),
                pltpu.VMEM((items, rows // ts, width * ts), jnp.bfloat16),
                pltpu.SMEM((xs * zs * CAPC,), jnp.int32),
                pltpu.SMEM((items,), jnp.int32),
                pltpu.SMEM((xs * zs,), jnp.int32),
                pltpu.SMEM((items,), jnp.int32),
                pltpu.SemaphoreType.DMA((items,)),
                pltpu.SemaphoreType.DMA((items,)),
                pltpu.SemaphoreType.DMA((2,)),
            ],
            compiler_params=pltpu.CompilerParams(vmem_limit_bytes=VMEM),
            cost_estimate=pl.CostEstimate(
                flops=10**9, bytes_accessed=2 * items * rows * width, transcendentals=0
            ),
        )(my_z, slot_of_prompt, prompt_of, *moved, *more)

    out = join(BOUNDS[:-1], moved[:-1], None)
    return join(BOUNDS[-2:], moved[-1:], out)


def solution(mesh):
    groups, tensors = mesh.devices.shape
    grid = Mesh(
        mesh.devices.reshape(groups // GROUPS_Z, GROUPS_Z, tensors), ("x", "z", "t")
    )
    split = P(("x", "z"), None, "t")
    return jax.shard_map(
        steps,
        mesh=grid,
        in_specs=(split, split, split, P(), P(("x", "z")), P(("x", "z"))),
        out_specs=P(("x", "z"), "t", None),
        check_vma=False,
    )
```
